32 devices in a mesh: tile: 8 (over z, y), band: 4 (over x, core).
Axes of the slice: x: 2, y: 2, z: 4, core: 2. Of those that a mesh axis runs over, the one named last changes fastest.
Arguments:
- observed: float32 [96, 4096, 128], P('band', 'tile'), may hold values from 0 to 4
- weights: float32 [96, 4096, 128], P('band', 'tile'), may hold values from 0.2 to 6, as said below
- morphology: float32 [4, 4096, 128], P(None, 'tile'), may hold values from 0 to 1
- spectra: float32 [4, 96, 2048], P(None, 'band', 'tile'), may hold values from 0.2 to 2
- blend_blocks: int32 [8, 256], P('tile'), may hold values from 1 to 4, 512 in all within a row
- source_count: int32 [2048], P('tile'), may hold values from 1 to 4
- sent_blocks: int32 [8, 8, 4], P('tile'), may hold values from 0 to 512, as said below
- landing_blocks: int32 [8, 8, 4], P('tile'), may hold values from 0 to 512, as said below
Outputs:
- new_morphology: float32 [4, 4096, 128], P(None, 'tile')
- new_spectra: float32 [4, 96, 2048], P(None, 'band', 'tile')
- misfit: float32 [2048], P('tile')
The draws below stay inside these ranges and needn't reach their ends.
Inputs may be any that keep to these rules, and one draw needn't show every extreme that they name: `weights`: Positive. `sent_blocks`: entry [s, d, j] is a block of tile index s whose model margins a block of tile index d, or 512 for an empty slot; at most 4 live slots from one sender to one receiver, the live ones first; every sender fills all 4 slots to some receiver and every receiver gets all 4 from some sender; a block may appear in several slots. `landing_blocks`: entry [d, s, j] is the block of tile index d on which slot j from sender s lands, or 512 exactly where sent_blocks[s, d, j] is 512; several slots may land on one block.
All inputs are finite; a program needn't handle non-finite values.
Results may differ from the reference program's by a relative error of at most 0.0003.
Values sent between devices are 32-bit elements; how exact they have to be, the bound alone decides.
A program may use at most 128 MiB of HBM per device.

```python
import math
import jax
import jax.numpy as jnp
import numpy as np
from jax import lax

PIX = 128
SOURCES = 4
CAP = 4
ITERS = 2
BLK_DEV = 512
BLEND_DEV = 256
CHAN = 96
BLOCKS = 4096
BLENDS = 2048
N_TILE = 8


def link_tables(key):
    base = jax.random.fold_in(key, 7)
    count_key, from_key, land_key = jax.random.split(base, 3)
    counts = jax.random.randint(count_key, (N_TILE, N_TILE), 0, CAP + 1)
    rows = jnp.arange(N_TILE)
    successor = rows[None, :] == (rows[:, None] + 1) % N_TILE
    counts = jnp.where(successor, CAP, counts)
    slot_index = jnp.arange(CAP)
    live_from = slot_index[None, None, :] < counts[:, :, None]
    sent_rows = jnp.where(live_from, jax.random.randint(from_key, (N_TILE, N_TILE, CAP), 0, BLK_DEV), BLK_DEV)
    land_rows = jnp.where(jnp.transpose(live_from, (1, 0, 2)), jax.random.randint(land_key, (N_TILE, N_TILE, CAP), 0, BLK_DEV), BLK_DEV)
    return (sent_rows.astype(jnp.int32), land_rows.astype(jnp.int32))


def draw_sent_blocks(key, part):
    return link_tables(key)[0]


def draw_landing_blocks(key, part):
    return link_tables(key)[1]


def draw_weights(key, part):
    ramp = jnp.exp(jnp.log(3.0) * jnp.arange(CHAN, dtype=jnp.float32) / max(CHAN - 1, 1))
    noise = jnp.exp(jax.random.uniform(key, (CHAN, BLOCKS, PIX), jnp.float32, jnp.log(0.5), jnp.log(2.0)))
    return (ramp[:, None, None] * noise).astype(jnp.float32)


def with_ends(values, rng, least, top_value):
    index_at = [jax.random.randint(jax.random.fold_in(rng, axis), (), 0, length) for axis, length in enumerate(values.shape)]
    main_axis = values.shape.index(max(values.shape))
    next_to = index_at[:main_axis] + [(index_at[main_axis] + 1) % values.shape[main_axis]] + index_at[main_axis + 1:]
    return values.at[tuple(index_at)].set(least).at[tuple(next_to)].set(top_value)


def steps_of(rng, extent, pieces, least, top_value):
    def one(dim, blocks):
        steps = jax.random.uniform(jax.random.fold_in(jax.random.fold_in(rng, 6), dim), (blocks,), jnp.float32, least / len(pieces), top_value / len(pieces))
        return jnp.repeat(jnp.exp(steps), extent[dim] // blocks).reshape((-1,) + (1,) * (len(extent) - dim - 1))

    loudness = one(*pieces[0])
    for cut in pieces[1:]:
        loudness = loudness * one(*cut)
    return loudness


def length_profile(count, total, limit, skew):
    weights = [(1 << 20) // math.isqrt(standing ** skew) + 1 for standing in range(2, count + 1)]
    surplus, holding = total - limit - (count - 1), [1] * (count - 1)
    while surplus > 0:
        movable = [i for i in range(count - 1) if holding[i] < limit]
        pool, remaining = sum([weights[i] for i in movable]), surplus
        for i in movable:
            addition = min(limit - holding[i], max(1, remaining * weights[i] // pool), surplus)
            holding[i] = holding[i] + addition
            surplus = surplus - addition
    return np.array([limit] + holding)


def ragged(stream_key, amount, total, most, slope):
    if amount == 2:
        one = jax.random.randint(stream_key, (), max(1, total - most), min(most, total - 1) + 1)
        return jnp.stack([one, total - one])
    lengths = jnp.asarray(length_profile(amount, total, most, slope), jnp.int32)
    pairs = (amount - 1) // 2
    donor, sink = lengths[1:1 + 2 * pairs:2], lengths[2:2 + 2 * pairs:2]
    slack = jnp.minimum(donor - 1, most - sink)
    passed = jax.random.randint(jax.random.fold_in(stream_key, 1), (pairs,), 0, 1 << 20) % (slack + 1)
    lengths = lengths.at[1:1 + 2 * pairs:2].set(donor - passed).at[2:2 + 2 * pairs:2].set(sink + passed)
    return lengths[jax.random.permutation(jax.random.fold_in(stream_key, 2), amount)]


def setup_inputs(seed: int = 0) -> dict:
    seeds = jax.random.split(jax.random.key(seed), 9)
    observed = jnp.clip(4.0 * jax.random.uniform(seeds[0], (CHAN, BLOCKS, PIX), jnp.float32) ** steps_of(seeds[0], (CHAN, BLOCKS, PIX), ((0, 4), (1, 8)), -0.2, 0.2), 0.0, 4.0)
    weights = draw_weights(jax.random.fold_in(seeds[8], 71), 0)
    morphology = jnp.clip(1.0 * jax.random.uniform(seeds[2], (SOURCES, BLOCKS, PIX), jnp.float32) ** steps_of(seeds[2], (SOURCES, BLOCKS, PIX), ((1, 8),), -0.2, 0.2), 0.0, 1.0)
    spectra = jnp.clip(jnp.exp(math.log(2.0) - 2.3025851 * jax.random.uniform(seeds[3], (SOURCES, CHAN, BLENDS), jnp.float32) ** steps_of(seeds[3], (SOURCES, CHAN, BLENDS), ((1, 4), (2, 8)), -0.2, 0.2)), 0.2, 2.0)
    blend_blocks = jax.vmap(lambda own: ragged(own, BLEND_DEV, BLK_DEV, 4, 1))(jax.random.split(seeds[4], N_TILE)).reshape((N_TILE, BLEND_DEV)).astype(jnp.int32)
    source_count = with_ends(jax.random.randint(seeds[5], (BLENDS,), 1, SOURCES + 1), jax.random.fold_in(seeds[5], 1), 1, SOURCES).astype(jnp.int32)
    sent_blocks = draw_sent_blocks(jax.random.fold_in(seeds[8], 71), 0)
    landing_blocks = draw_landing_blocks(jax.random.fold_in(seeds[8], 71), 0)
    return {"observed": observed, "weights": weights, "morphology": morphology, "spectra": spectra, "blend_blocks": blend_blocks, "source_count": source_count, "sent_blocks": sent_blocks, "landing_blocks": landing_blocks}


HIGH = lax.Precision.HIGHEST


def reference(observed, weights, morphology, spectra, blend_blocks, source_count, sent_blocks, landing_blocks):
    block_ends = jnp.cumsum(blend_blocks, axis=1)
    position = jnp.arange(BLK_DEV, dtype=jnp.int32)
    local_blend = jnp.sum((block_ends[:, None, :] <= position[None, :, None]).astype(jnp.int32), axis=2)
    tile_base = jnp.arange(N_TILE, dtype=jnp.int32)
    block_blend = (local_blend + BLEND_DEV * tile_base[:, None]).reshape(-1).astype(jnp.int32)
    alive_slots = (jnp.arange(SOURCES, dtype=jnp.int32)[:, None] < source_count[None, :]).astype(jnp.float32)
    alive_blocks = alive_slots[:, block_blend]
    shape_now = morphology * alive_blocks[:, :, None]
    color_now = spectra * alive_slots[:, None, :]
    source_live = sent_blocks < BLK_DEV
    source_global = jnp.where(source_live, tile_base[:, None, None] * BLK_DEV + sent_blocks, BLOCKS).reshape(-1).astype(jnp.int32)
    landing_turned = jnp.transpose(landing_blocks, (1, 0, 2))
    target_global = jnp.where(landing_turned < BLK_DEV, tile_base[None, :, None] * BLK_DEV + landing_turned, BLOCKS).reshape(-1).astype(jnp.int32)
    misfit = jnp.zeros((BLENDS,), jnp.float32)
    for iteration in range(ITERS):
        color_blocks = color_now[:, :, block_blend]
        own_model = jnp.einsum('kcb,kbp->cbp', color_blocks, shape_now, precision=HIGH)
        incoming = jnp.take(own_model, source_global, axis=1, mode="fill", fill_value=0.0)
        full_model = own_model.at[:, target_global].add(incoming, mode="drop")
        residual = full_model - observed
        weighted = weights * residual
        misfit = jax.ops.segment_sum(jnp.sum(weighted * residual, axis=(0, 2)), block_blend, num_segments=BLENDS)
        returning = jnp.take(weighted, target_global, axis=1, mode="fill", fill_value=0.0)
        adjoint = weighted.at[:, source_global].add(returning, mode="drop")
        grad_shape = jnp.einsum('kcb,cbp->kbp', color_blocks, adjoint, precision=HIGH)
        per_block = jnp.einsum('kbp,cbp->bkc', shape_now, adjoint, precision=HIGH)
        grad_color = jnp.transpose(jax.ops.segment_sum(per_block, block_blend, num_segments=BLENDS), (1, 2, 0))
        color_power = jnp.sum(color_now * color_now, axis=1)
        step_shape = 1.0 / (1.0 + color_power[:, block_blend])
        shape_power = jax.ops.segment_sum(jnp.sum(shape_now * shape_now, axis=2).T, block_blend, num_segments=BLENDS).T
        step_color = 1.0 / (1.0 + shape_power)
        shape_next = jnp.maximum(shape_now - step_shape[:, :, None] * grad_shape, 0.0) * alive_blocks[:, :, None]
        color_now = jnp.maximum(color_now - step_color[:, None, :] * grad_color, 0.0) * alive_slots[:, None, :]
        shape_now = shape_next
    return shape_now, color_now, misfit
```

```python
import functools
import jax
import jax.numpy as jnp
from jax import lax
from jax.experimental import pallas as pl
from jax.experimental.pallas import tpu as pltpu
from jax.sharding import PartitionSpec as P

ITERS = 2
LANES = 128
SUB = 8
MESH = pl.DeviceIdType.MESH
VM = pl.BlockSpec(memory_space=pltpu.VMEM)
F32 = jnp.float32
BF = jnp.bfloat16


def split2(x):
    hi = x.astype(BF)
    return hi, (x - hi.astype(F32)).astype(BF)


def split3(x):
    hi = x.astype(BF)
    rest = x - hi.astype(F32)
    mid = rest.astype(BF)
    return hi, mid, (rest - mid.astype(F32)).astype(BF)


NN = ((1,), (0,))
NT = ((1,), (1,))
TN = ((0,), (0,))


def select_dot(x, onehot, dims):
    out = None
    for piece in split3(x):
        part = lax.dot_general(piece, onehot, (dims, ((), ())), preferred_element_type=F32)
        out = part if out is None else out + part
    return out


def pick_dot(onehot, x):
    out = None
    for piece in split3(x):
        part = lax.dot_general(onehot, piece, (NT, ((), ())), preferred_element_type=F32)
        out = part if out is None else out + part
    return out


def write_packets(sent_ref, shape_ref, cb_ref, pkt_ref):
    sources = shape_ref.shape[0]
    slots = pkt_ref.shape[0]
    pkt_ref[...] = jnp.zeros_like(pkt_ref)
    sent = sent_ref[...]
    for k in range(sources):
        pkt_ref[:, k, :] = pick_dot(sent, shape_ref[k])[:slots]
    pkt_ref[:, sources, :] = pick_dot(sent, cb_ref[...])[:slots]


def start_kernel(chan, sent_ref, morph_ref, spec_ref, len_ref, cnt_ref,
                 shape_ref, color_ref, cb_ref, memt_ref, cntb_ref, amask_ref, pkt_ref):
    sources, blocks, _ = morph_ref.shape
    blends = len_ref.shape[1]
    lengths = jnp.broadcast_to(len_ref[...].astype(F32), (SUB, blends))
    rows = lax.broadcasted_iota(jnp.int32, (blends, blends), 0)
    cols = lax.broadcasted_iota(jnp.int32, (blends, blends), 1)
    ends = jnp.dot(lengths.astype(BF), (rows <= cols).astype(F32).astype(BF), preferred_element_type=F32)
    starts = ends - lengths
    pos = lax.broadcasted_iota(jnp.int32, (blocks, blends), 0).astype(F32)
    memt = jnp.where((pos >= starts[0:1]) & (pos < ends[0:1]), 1.0, 0.0).astype(BF)
    memt_ref[...] = memt
    count = jnp.broadcast_to(cnt_ref[...].astype(F32), (SUB, blends))
    count_b = lax.dot_general(count.astype(BF), memt, (NT, ((), ())), preferred_element_type=F32)
    cntb_ref[...] = count_b
    row = lax.broadcasted_iota(jnp.int32, (LANES, blends), 0)
    amask = jnp.where(((row // chan).astype(F32) < count[0:1]) & (row < chan * sources), 1.0, 0.0)
    amask_ref[...] = amask
    color = spec_ref[...] * amask
    color_ref[...] = color
    cb_ref[...] = select_dot(color, memt, NT)
    for k in range(sources):
        shape_ref[k] = jnp.transpose(morph_ref[k]) * jnp.where(count_b[0:1] > k, 1.0, 0.0)
    write_packets(sent_ref, shape_ref, cb_ref, pkt_ref)


def exchange_kernel(tiles, src_ref, out_ref, land, send_sem, recv_sem):
    me = lax.axis_index("tile")
    slots = src_ref.shape[0] // tiles
    barrier = pltpu.get_barrier_semaphore()
    for o in range(1, tiles):
        pl.semaphore_signal(barrier, inc=1, device_id={"tile": lax.rem(me + o, tiles)}, device_id_type=MESH)
    pl.semaphore_wait(barrier, tiles - 1)
    copies = []
    for o in range(1, tiles):
        to = lax.rem(me + o, tiles)
        copy = pltpu.make_async_remote_copy(
            src_ref=src_ref.at[pl.ds(to * slots, slots)],
            dst_ref=land.at[pl.ds(me * slots, slots)],
            send_sem=send_sem.at[o], recv_sem=recv_sem.at[o],
            device_id={"tile": to}, device_id_type=MESH)
        copy.start()
        copies.append(copy)
    land[pl.ds(me * slots, slots)] = src_ref[pl.ds(me * slots, slots)]
    for o in range(1, tiles):
        frm = lax.rem(me - o + tiles, tiles)
        pltpu.make_async_remote_copy(
            src_ref=src_ref.at[pl.ds(frm * slots, slots)],
            dst_ref=land.at[pl.ds(frm * slots, slots)],
            send_sem=send_sem.at[o], recv_sem=recv_sem.at[o],
            device_id={"tile": frm}, device_id_type=MESH).wait_recv()
    out_ref[...] = land[...]
    for copy in copies:
        copy.wait_send()


def exchange(packets, tiles, cid):
    return pl.pallas_call(
        functools.partial(exchange_kernel, tiles),
        out_shape=jax.ShapeDtypeStruct(packets.shape, F32),
        in_specs=[VM], out_specs=VM,
        scratch_shapes=[pltpu.VMEM(packets.shape, F32), pltpu.SemaphoreType.DMA((tiles,)),
                        pltpu.SemaphoreType.DMA((tiles,))],
        compiler_params=pltpu.CompilerParams(collective_id=cid, has_side_effects=True),
    )(packets)


def fold(x):
    return jnp.sum(x.reshape(x.shape[0] // SUB, SUB, x.shape[1]), axis=0)


def column(ref, index, rows):
    return jnp.broadcast_to(ref[pl.ds(index, 1), :], (rows, LANES))


def main_kernel(sources, hit_ref, recv_ref, obs_ref, wts_ref, shape_ref, cb_ref,
                grad_ref, pb_ref, aux_ref, ret_ref, incm, adjs, wtt, wl, pbs, vsh, vcol, mis, vpb):
    chan, rows, pixels = obs_ref.shape
    slots = recv_ref.shape[0]
    step = pl.program_id(0)
    kc = sources * chan
    deep = 32

    @pl.when(step == 0)
    def _():
        wl[...] = jnp.zeros_like(wl)

        def padded(x):
            if slots < LANES:
                x = jnp.concatenate([x, jnp.zeros((LANES - slots, LANES), F32)], axis=0)
            return jnp.transpose(x)

        for k in range(sources):
            vsh[k] = padded(recv_ref[:, k, :])
        vcol[...] = padded(recv_ref[:, sources, :])
        for c in range(chan):
            own = None
            for k in range(sources):
                term = column(vcol, k * chan + c, pixels) * vsh[k]
                own = term if own is None else own + term
            hi, lo = split2(own)
            incm[c] = jnp.concatenate([hi, lo], axis=1)

    hit = hit_ref[...]
    hit2 = jnp.concatenate([hit, hit], axis=0)
    for c in range(chan):
        inc = jnp.dot(incm[c], hit2, preferred_element_type=F32)
        adjs[c] = inc - jnp.transpose(obs_ref[c])
        wtt[c] = jnp.transpose(wts_ref[c])
    pbs[...] = jnp.zeros_like(pbs)
    mis[...] = jnp.zeros_like(mis)

    def slab(g, carry):
        at = pl.ds(pl.multiple_of(g * deep, deep), deep)
        sh = [shape_ref[k, at, :] for k in range(sources)]
        grads = [None] * sources
        for c in range(chan):
            cols = [column(cb_ref, k * chan + c, deep) for k in range(sources)]
            own = adjs[c, at, :]
            for k in range(sources):
                own = own + cols[k] * sh[k]
            adj = wtt[c, at, :] * own
            adjs[c, at, :] = adj
            mis[0] += fold(adj * own)
            for k in range(sources):
                term = cols[k] * adj
                grads[k] = term if grads[k] is None else grads[k] + term
                pbs[k * chan + c] += fold(sh[k] * adj)
        for k in range(sources):
            grad_ref[k, at, :] = grads[k]
            mis[1 + k] += fold(sh[k] * sh[k])
        return carry

    lax.fori_loop(0, pixels // deep, slab, 0)
    pb_ref[...] = jnp.zeros_like(pb_ref)
    pb_ref[pl.ds(0, kc), :] = jnp.sum(pbs[...], axis=1)
    aux_ref[...] = jnp.zeros_like(aux_ref)
    total = jnp.sum(mis[...], axis=1)
    aux_ref[pl.ds(sources, 1), :] = total[0:1]
    aux_ref[pl.ds(SUB, sources), :] = total[1:1 + sources]
    for k in range(sources):
        mine = cb_ref[pl.ds(k * chan, chan), :]
        aux_ref[pl.ds(k, 1), :] = jnp.sum(mine * mine, axis=0, keepdims=True)
    hit_wide = jnp.concatenate([hit, hit], axis=1)
    for c in range(chan):
        hi, lo = split2(adjs[c])
        wl[c] += lax.dot_general(jnp.concatenate([hi, lo], axis=1), hit_wide, (NT, ((), ())),
                                 preferred_element_type=F32)

    @pl.when(step == pl.num_programs(0) - 1)
    def _():
        ret_ref[...] = jnp.zeros_like(ret_ref)
        vpb[...] = jnp.zeros_like(vpb)
        pbs[...] = jnp.zeros_like(pbs)

        def back(g, carry):
            at = pl.ds(pl.multiple_of(g * deep, deep), deep)
            sh = [vsh[k, at, :] for k in range(sources)]
            grads = [None] * sources
            for c in range(chan):
                adj = wl[c, at, :]
                for k in range(sources):
                    term = column(vcol, k * chan + c, deep) * adj
                    grads[k] = term if grads[k] is None else grads[k] + term
                    pbs[k * chan + c] += fold(sh[k] * adj)
            for k in range(sources):
                vsh[k, at, :] = grads[k]
            return carry

        lax.fori_loop(0, pixels // deep, back, 0)
        vpb[pl.ds(0, kc), :] = jnp.sum(pbs[...], axis=1)
        for k in range(sources):
            ret_ref[:, k, :] = jnp.transpose(vsh[k])[:slots]
        ret_ref[:, sources, :] = jnp.transpose(vpb[...])[:slots]


def main_pass(hit, recv, observed, weights, shape_now, cb):
    sources, pixels, blocks = shape_now.shape
    chan = observed.shape[0]
    slots = recv.shape[0]
    rows = LANES
    big = pl.BlockSpec((chan, rows, pixels), lambda i: (0, i, 0))
    whole = pl.BlockSpec(recv.shape, lambda i: (0, 0, 0))
    table = pl.BlockSpec((LANES, rows), lambda i: (0, i))
    shp = pl.BlockSpec((sources, pixels, rows), lambda i: (0, 0, i))
    sds = jax.ShapeDtypeStruct
    slab = pltpu.VMEM((chan, pixels, LANES), F32)
    return pl.pallas_call(
        functools.partial(main_kernel, sources),
        grid=(blocks // rows,),
        in_specs=[table, whole, big, big, shp, table],
        out_specs=[shp, table, pl.BlockSpec((2 * SUB, rows), lambda i: (0, i)), whole],
        out_shape=[sds(shape_now.shape, F32), sds((LANES, blocks), F32), sds((2 * SUB, blocks), F32),
                   sds(recv.shape, F32)],
        scratch_shapes=[pltpu.VMEM((chan, pixels, 2 * LANES), BF), slab, slab, slab,
                        pltpu.VMEM((sources * chan, SUB, LANES), F32),
                        pltpu.VMEM((sources, pixels, LANES), F32), pltpu.VMEM((LANES, LANES), F32),
                        pltpu.VMEM((SUB, SUB, LANES), F32), pltpu.VMEM((LANES, LANES), F32)],
        compiler_params=pltpu.CompilerParams(dimension_semantics=("arbitrary",)),
    )(hit, recv, observed, weights, shape_now, cb)


def fix_kernel(chan, sent_ref, back_ref, grad_ref, pb_ref, aux_ref, memt_ref, color_ref, amask_ref,
               gout_ref, auxt_ref, cnext_ref):
    sources = grad_ref.shape[0]
    slots = back_ref.shape[0]
    sent = sent_ref[...][:slots]
    for k in range(sources):
        gout_ref[k] = grad_ref[k] + select_dot(back_ref[:, k, :], sent, TN)
    per_block = pb_ref[...] + select_dot(back_ref[:, sources, :], sent, TN)
    auxt_ref[...] = aux_ref[pl.ds(0, SUB), :]
    memt = memt_ref[...]
    grad_color = select_dot(per_block, memt, NN)
    powers = select_dot(aux_ref[pl.ds(SUB, SUB), :], memt, NN)
    row = lax.broadcasted_iota(jnp.int32, color_ref.shape, 0) // chan
    power = jnp.zeros(color_ref.shape, F32)
    for k in range(sources):
        power = jnp.where(row == k, powers[k:k + 1], power)
    cnext_ref[...] = jnp.maximum(color_ref[...] - grad_color / (1.0 + power), 0.0) * amask_ref[...]


def reduce_kernel(bands, parts, g_ref, a_ref, gout_ref, aout_ref, r1, r2, r3, ar,
                  s1, v1, s2, v2, s3, v3, sa, va):
    me = lax.axis_index("band")
    core = lax.rem(me, 2)
    x = me // 2
    chips = bands // 2
    partner = x * 2 + 1 - core
    half = g_ref.shape[1] // 2
    rows = half // parts
    barrier = pltpu.get_barrier_semaphore()
    for o in range(1, bands):
        pl.semaphore_signal(barrier, inc=1, device_id={"band": lax.rem(me + o, bands)}, device_id_type=MESH)
    pl.semaphore_wait(barrier, bands - 1)

    def chunk(c, q):
        return pl.ds(pl.multiple_of(c * half + q * rows, SUB), rows)

    sends = []
    for q in range(parts):
        copy = pltpu.make_async_remote_copy(
            src_ref=g_ref.at[:, chunk(1 - core, q), :], dst_ref=r1.at[q],
            send_sem=s1.at[q], recv_sem=v1.at[q], device_id={"band": partner}, device_id_type=MESH)
        copy.start()
        sends.append(copy)
    first = list(sends)
    for o in range(1, bands):
        to = lax.rem(me + o, bands)
        copy = pltpu.make_async_remote_copy(
            src_ref=a_ref, dst_ref=ar.at[me], send_sem=sa.at[o], recv_sem=va.at[o],
            device_id={"band": to}, device_id_type=MESH)
        copy.start()
        sends.append(copy)
    ar[me] = a_ref[...]
    for q in range(parts):
        first[q].wait_recv()
        r2[x, q] = g_ref[:, chunk(core, q), :] + r1[q]
        for o in range(1, chips):
            to = lax.rem(x + o, chips)
            copy = pltpu.make_async_remote_copy(
                src_ref=r2.at[x, q], dst_ref=r2.at[x, q], send_sem=s2.at[o, q], recv_sem=v2.at[o, q],
                device_id={"band": to * 2 + core}, device_id_type=MESH)
            copy.start()
            sends.append(copy)
    last = []
    for q in range(parts):
        for o in range(1, chips):
            frm = lax.rem(x - o + chips, chips)
            pltpu.make_async_remote_copy(
                src_ref=r2.at[frm, q], dst_ref=r2.at[frm, q], send_sem=s2.at[o, q], recv_sem=v2.at[o, q],
                device_id={"band": frm * 2 + core}, device_id_type=MESH).wait_recv()
        total = r2[0, q]
        for i in range(1, chips):
            total = total + r2[i, q]
        gout_ref[:, chunk(core, q), :] = total
        copy = pltpu.make_async_remote_copy(
            src_ref=gout_ref.at[:, chunk(core, q), :], dst_ref=r3.at[q],
            send_sem=s3.at[q], recv_sem=v3.at[q], device_id={"band": partner}, device_id_type=MESH)
        copy.start()
        last.append(copy)
    for o in range(1, bands):
        frm = lax.rem(me - o + bands, bands)
        pltpu.make_async_remote_copy(
            src_ref=a_ref, dst_ref=ar.at[frm], send_sem=sa.at[o], recv_sem=va.at[o],
            device_id={"band": frm}, device_id_type=MESH).wait_recv()
    total = ar[0]
    for i in range(1, bands):
        total = total + ar[i]
    aout_ref[...] = total
    for q in range(parts):
        last[q].wait_recv()
        gout_ref[:, chunk(1 - core, q), :] = r3[q]
    for copy in sends + last:
        copy.wait_send()


def band_sum(grad, auxt, bands, cid):
    sources, pixels, lanes = grad.shape
    parts = 4
    rows = pixels // 2 // parts
    chips = bands // 2
    dma = pltpu.SemaphoreType.DMA
    return pl.pallas_call(
        functools.partial(reduce_kernel, bands, parts),
        out_shape=[jax.ShapeDtypeStruct(grad.shape, F32), jax.ShapeDtypeStruct(auxt.shape, F32)],
        in_specs=[VM, VM], out_specs=[VM, VM],
        scratch_shapes=[pltpu.VMEM((parts, sources, rows, lanes), F32),
                        pltpu.VMEM((chips, parts, sources, rows, lanes), F32),
                        pltpu.VMEM((parts, sources, rows, lanes), F32),
                        pltpu.VMEM((bands,) + auxt.shape, F32),
                        dma((parts,)), dma((parts,)), dma((chips, parts)), dma((chips, parts)),
                        dma((parts,)), dma((parts,)), dma((bands,)), dma((bands,))],
        compiler_params=pltpu.CompilerParams(collective_id=cid, has_side_effects=True),
    )(grad, auxt)


def step_kernel(final, sent_ref, shape_ref, grad_ref, auxt_ref, cntb_ref, memt_ref, color_ref, *outs):
    sources = shape_ref.shape[0]
    snext_ref = outs[0]
    for k in range(sources):
        step = 1.0 / (1.0 + auxt_ref[pl.ds(k, 1), :])
        alive = jnp.where(cntb_ref[pl.ds(0, 1), :] > k, 1.0, 0.0)
        shape = jnp.maximum(shape_ref[k] - step * grad_ref[k], 0.0) * alive
        snext_ref[k] = jnp.transpose(shape) if final else shape
    if final:
        outs[1][...] = select_dot(auxt_ref[...], memt_ref[...], NN)
    else:
        outs[1][...] = select_dot(color_ref[...], memt_ref[...], NT)
        write_packets(sent_ref, snext_ref, outs[1], outs[2])


def on_device(
    observed, weights, morphology, spectra, blend_blocks, source_count, sent_blocks, landing_blocks
):
    chan, blocks, pixels = observed.shape
    sources = morphology.shape[0]
    blends = spectra.shape[2]
    tiles = lax.axis_size("tile")
    bands = lax.axis_size("band")
    slots = tiles * sent_blocks.shape[2]

    def onehot(index):
        index = jnp.pad(index.reshape(-1), (0, LANES - slots), constant_values=blocks)
        return (index[:, None] == jnp.arange(blocks, dtype=jnp.int32)[None, :]).astype(BF)

    sent = onehot(sent_blocks)
    hit = onehot(landing_blocks)
    spec2 = jnp.pad(spectra.reshape(sources * chan, blends), ((0, LANES - sources * chan), (0, 0)))
    sds = jax.ShapeDtypeStruct
    packet = sds((slots, SUB, LANES), F32)
    table = sds((LANES, blocks), F32)
    palette = sds((LANES, blends), F32)
    turned = sds((sources, pixels, blocks), F32)
    shape_now, color_now, cb, memt, cntb, amask, packets = pl.pallas_call(
        functools.partial(start_kernel, chan),
        in_specs=[VM] * 5, out_specs=[VM] * 7,
        out_shape=[turned, palette, table, sds((blocks, blends), BF), sds((SUB, blocks), F32), palette, packet],
    )(sent, morphology, spec2, blend_blocks, source_count.reshape(1, blends))
    for it in range(ITERS):
        recv = exchange(packets, tiles, 3 * it)
        grad, pb, aux, ret = main_pass(hit, recv, observed, weights, shape_now, cb)
        back = exchange(ret, tiles, 3 * it + 1)
        grad, auxt, color_now = pl.pallas_call(
            functools.partial(fix_kernel, chan),
            in_specs=[VM] * 8, out_specs=[VM] * 3,
            out_shape=[turned, sds((SUB, blocks), F32), palette],
        )(sent, back, grad, pb, aux, memt, color_now, amask)
        grad, auxt = band_sum(grad, auxt, bands, 3 * it + 2)
        final = it == ITERS - 1
        outs = [sds(morphology.shape, F32), sds((SUB, blends), F32)] if final else [turned, table, packet]
        results = pl.pallas_call(
            functools.partial(step_kernel, final),
            in_specs=[VM] * 7, out_specs=[VM] * len(outs), out_shape=outs,
        )(sent, shape_now, grad, auxt, cntb, memt, color_now)
        if not final:
            shape_now, cb, packets = results
    spectra_out = color_now[:sources * chan].reshape(sources, chan, blends)
    return (results[0], spectra_out, results[1][sources])


def solution(mesh):
    return jax.shard_map(
        on_device,
        mesh=mesh,
        in_specs=(
            P("band", "tile", None),
            P("band", "tile", None),
            P(None, "tile", None),
            P(None, "band", "tile"),
            P("tile", None),
            P("tile"),
            P("tile", None, None),
            P("tile", None, None),
        ),
        out_specs=(P(None, "tile", None), P(None, "band", "tile"), P("tile")),
        check_vma=False,
    )
```

```python
import functools
import jax
import jax.numpy as jnp
from jax import lax
from jax.experimental import pallas as pl
from jax.experimental.pallas import tpu as pltpu
from jax.sharding import PartitionSpec as P

ITERS = 2
LANES = 128
SUB = 8
MESH = pl.DeviceIdType.MESH
VM = pl.BlockSpec(memory_space=pltpu.VMEM)
F32 = jnp.float32
BF = jnp.bfloat16


def split2(x):
    hi = x.astype(BF)
    return hi, (x - hi.astype(F32)).astype(BF)


def split3(x):
    hi = x.astype(BF)
    rest = x - hi.astype(F32)
    mid = rest.astype(BF)
    return hi, mid, (rest - mid.astype(F32)).astype(BF)


NN = ((1,), (0,))
NT = ((1,), (1,))
TN = ((0,), (0,))


def select_dot(x, onehot, dims):
    out = None
    for piece in split3(x):
        part = lax.dot_general(piece, onehot, (dims, ((), ())), preferred_element_type=F32)
        out = part if out is None else out + part
    return out


def pick_dot(onehot, x):
    out = None
    for piece in split3(x):
        part = lax.dot_general(onehot, piece, (NT, ((), ())), preferred_element_type=F32)
        out = part if out is None else out + part
    return out


def write_packets(sent_ref, shape_ref, cb_ref, pkt_ref):
    sources = shape_ref.shape[0]
    slots = pkt_ref.shape[0]
    pkt_ref[...] = jnp.zeros_like(pkt_ref)
    sent = sent_ref[...]
    for k in range(sources):
        pkt_ref[:, k, :] = pick_dot(sent, shape_ref[k])[:slots]
    pkt_ref[:, sources, :] = pick_dot(sent, cb_ref[...])[:slots]


def start_kernel(chan, sent_ref, morph_ref, spec_ref, len_ref, cnt_ref,
                 shape_ref, color_ref, cb_ref, memt_ref, cntb_ref, amask_ref, pkt_ref):
    sources, blocks, _ = morph_ref.shape
    blends = len_ref.shape[1]
    lengths = jnp.broadcast_to(len_ref[...].astype(F32), (SUB, blends))
    rows = lax.broadcasted_iota(jnp.int32, (blends, blends), 0)
    cols = lax.broadcasted_iota(jnp.int32, (blends, blends), 1)
    ends = jnp.dot(lengths.astype(BF), (rows <= cols).astype(F32).astype(BF), preferred_element_type=F32)
    starts = ends - lengths
    pos = lax.broadcasted_iota(jnp.int32, (blocks, blends), 0).astype(F32)
    memt = jnp.where((pos >= starts[0:1]) & (pos < ends[0:1]), 1.0, 0.0).astype(BF)
    memt_ref[...] = memt
    count = jnp.broadcast_to(cnt_ref[...].astype(F32), (SUB, blends))
    count_b = lax.dot_general(count.astype(BF), memt, (NT, ((), ())), preferred_element_type=F32)
    cntb_ref[...] = count_b
    row = lax.broadcasted_iota(jnp.int32, (LANES, blends), 0)
    amask = jnp.where(((row // chan).astype(F32) < count[0:1]) & (row < chan * sources), 1.0, 0.0)
    amask_ref[...] = amask
    color = spec_ref[...] * amask
    color_ref[...] = color
    cb_ref[...] = select_dot(color, memt, NT)
    for k in range(sources):
        shape_ref[k] = jnp.transpose(morph_ref[k]) * jnp.where(count_b[0:1] > k, 1.0, 0.0)
    write_packets(sent_ref, shape_ref, cb_ref, pkt_ref)


def exchange_kernel(tiles, src_ref, out_ref, land, send_sem, recv_sem):
    me = lax.axis_index("tile")
    slots = src_ref.shape[0] // tiles
    barrier = pltpu.get_barrier_semaphore()
    for o in range(1, tiles):
        pl.semaphore_signal(barrier, inc=1, device_id={"tile": lax.rem(me + o, tiles)}, device_id_type=MESH)
    pl.semaphore_wait(barrier, tiles - 1)
    copies = []
    for o in range(1, tiles):
        to = lax.rem(me + o, tiles)
        copy = pltpu.make_async_remote_copy(
            src_ref=src_ref.at[pl.ds(to * slots, slots)],
            dst_ref=land.at[pl.ds(me * slots, slots)],
            send_sem=send_sem.at[o], recv_sem=recv_sem.at[o],
            device_id={"tile": to}, device_id_type=MESH)
        copy.start()
        copies.append(copy)
    land[pl.ds(me * slots, slots)] = src_ref[pl.ds(me * slots, slots)]
    for o in range(1, tiles):
        frm = lax.rem(me - o + tiles, tiles)
        pltpu.make_async_remote_copy(
            src_ref=src_ref.at[pl.ds(frm * slots, slots)],
            dst_ref=land.at[pl.ds(frm * slots, slots)],
            send_sem=send_sem.at[o], recv_sem=recv_sem.at[o],
            device_id={"tile": frm}, device_id_type=MESH).wait_recv()
    out_ref[...] = land[...]
    for copy in copies:
        copy.wait_send()


def exchange(packets, tiles, cid):
    return pl.pallas_call(
        functools.partial(exchange_kernel, tiles),
        out_shape=jax.ShapeDtypeStruct(packets.shape, F32),
        in_specs=[VM], out_specs=VM,
        scratch_shapes=[pltpu.VMEM(packets.shape, F32), pltpu.SemaphoreType.DMA((tiles,)),
                        pltpu.SemaphoreType.DMA((tiles,))],
        compiler_params=pltpu.CompilerParams(collective_id=cid, has_side_effects=True),
    )(packets)


def fold(x):
    return jnp.sum(x.reshape(x.shape[0] // SUB, SUB, x.shape[1]), axis=0)


def column(ref, index, rows):
    return jnp.broadcast_to(ref[pl.ds(index, 1), :], (rows, LANES))


def main_kernel(sources, hit_ref, recv_ref, obs_ref, wts_ref, shape_ref, cb_ref,
                grad_ref, pb_ref, aux_ref, ret_ref, incm, adjs, wtt, wl, pbs, vsh, vcol, mis, vpb):
    chan, rows, pixels = obs_ref.shape
    slots = recv_ref.shape[0]
    step = pl.program_id(0)
    kc = sources * chan
    deep = 32

    @pl.when(step == 0)
    def _():
        wl[...] = jnp.zeros_like(wl)

        def padded(x):
            if slots < LANES:
                x = jnp.concatenate([x, jnp.zeros((LANES - slots, LANES), F32)], axis=0)
            return jnp.transpose(x)

        for k in range(sources):
            vsh[k] = padded(recv_ref[:, k, :])
        vcol[...] = padded(recv_ref[:, sources, :])
        for c in range(chan):
            own = None
            for k in range(sources):
                term = column(vcol, k * chan + c, pixels) * vsh[k]
                own = term if own is None else own + term
            hi, lo = split2(own)
            incm[c] = jnp.concatenate([hi, lo], axis=1)

    hit = hit_ref[...]
    hit2 = jnp.concatenate([hit, hit], axis=0)
    for c in range(chan):
        inc = jnp.dot(incm[c], hit2, preferred_element_type=F32)
        adjs[c] = inc - jnp.transpose(obs_ref[c])
        wtt[c] = jnp.transpose(wts_ref[c])
    pbs[...] = jnp.zeros_like(pbs)
    mis[...] = jnp.zeros_like(mis)

    def slab(g, carry):
        at = pl.ds(pl.multiple_of(g * deep, deep), deep)
        sh = [shape_ref[k, at, :] for k in range(sources)]
        grads = [None] * sources
        for c in range(chan):
            cols = [column(cb_ref, k * chan + c, deep) for k in range(sources)]
            own = adjs[c, at, :]
            for k in range(sources):
                own = own + cols[k] * sh[k]
            adj = wtt[c, at, :] * own
            adjs[c, at, :] = adj
            mis[0] += fold(adj * own)
            for k in range(sources):
                term = cols[k] * adj
                grads[k] = term if grads[k] is None else grads[k] + term
                pbs[k * chan + c] += fold(sh[k] * adj)
        for k in range(sources):
            grad_ref[k, at, :] = grads[k]
            mis[1 + k] += fold(sh[k] * sh[k])
        return carry

    lax.fori_loop(0, pixels // deep, slab, 0)
    pb_ref[...] = jnp.zeros_like(pb_ref)
    pb_ref[pl.ds(0, kc), :] = jnp.sum(pbs[...], axis=1)
    aux_ref[...] = jnp.zeros_like(aux_ref)
    total = jnp.sum(mis[...], axis=1)
    aux_ref[pl.ds(sources, 1), :] = total[0:1]
    aux_ref[pl.ds(SUB, sources), :] = total[1:1 + sources]
    for k in range(sources):
        mine = cb_ref[pl.ds(k * chan, chan), :]
        aux_ref[pl.ds(k, 1), :] = jnp.sum(mine * mine, axis=0, keepdims=True)
    hit_wide = jnp.concatenate([hit, hit], axis=1)
    for c in range(chan):
        hi, lo = split2(adjs[c])
        wl[c] += lax.dot_general(jnp.concatenate([hi, lo], axis=1), hit_wide, (NT, ((), ())),
                                 preferred_element_type=F32)

    @pl.when(step == pl.num_programs(0) - 1)
    def _():
        ret_ref[...] = jnp.zeros_like(ret_ref)
        vpb[...] = jnp.zeros_like(vpb)
        pbs[...] = jnp.zeros_like(pbs)

        def back(g, carry):
            at = pl.ds(pl.multiple_of(g * deep, deep), deep)
            sh = [vsh[k, at, :] for k in range(sources)]
            grads = [None] * sources
            for c in range(chan):
                adj = wl[c, at, :]
                for k in range(sources):
                    term = column(vcol, k * chan + c, deep) * adj
                    grads[k] = term if grads[k] is None else grads[k] + term
                    pbs[k * chan + c] += fold(sh[k] * adj)
            for k in range(sources):
                vsh[k, at, :] = grads[k]
            return carry

        lax.fori_loop(0, pixels // deep, back, 0)
        vpb[pl.ds(0, kc), :] = jnp.sum(pbs[...], axis=1)
        for k in range(sources):
            ret_ref[:, k, :] = jnp.transpose(vsh[k])[:slots]
        ret_ref[:, sources, :] = jnp.transpose(vpb[...])[:slots]


def main_pass(hit, recv, observed, weights, shape_now, cb):
    sources, pixels, blocks = shape_now.shape
    chan = observed.shape[0]
    slots = recv.shape[0]
    rows = LANES
    big = pl.BlockSpec((chan, rows, pixels), lambda i: (0, i, 0))
    whole = pl.BlockSpec(recv.shape, lambda i: (0, 0, 0))
    table = pl.BlockSpec((LANES, rows), lambda i: (0, i))
    shp = pl.BlockSpec((sources, pixels, rows), lambda i: (0, 0, i))
    sds = jax.ShapeDtypeStruct
    slab = pltpu.VMEM((chan, pixels, LANES), F32)
    return pl.pallas_call(
        functools.partial(main_kernel, sources),
        grid=(blocks // rows,),
        in_specs=[table, whole, big, big, shp, table],
        out_specs=[shp, table, pl.BlockSpec((2 * SUB, rows), lambda i: (0, i)), whole],
        out_shape=[sds(shape_now.shape, F32), sds((LANES, blocks), F32), sds((2 * SUB, blocks), F32),
                   sds(recv.shape, F32)],
        scratch_shapes=[pltpu.VMEM((chan, pixels, 2 * LANES), BF), slab, slab, slab,
                        pltpu.VMEM((sources * chan, SUB, LANES), F32),
                        pltpu.VMEM((sources, pixels, LANES), F32), pltpu.VMEM((LANES, LANES), F32),
                        pltpu.VMEM((SUB, SUB, LANES), F32), pltpu.VMEM((LANES, LANES), F32)],
        compiler_params=pltpu.CompilerParams(dimension_semantics=("arbitrary",)),
    )(hit, recv, observed, weights, shape_now, cb)


def reduce_kernel(tiles, bands, parts, src_ref, g_ref, a_ref, gout_ref, aout_ref, sum_ref, own_ref,
                  r1, r2, r3, ar, land, b1, b2, s1, v1, s2, v2, s3, v3, sa, va, st, vt, sb, vb, sc, vc):
    spot = lax.axis_index("tile")
    slots = src_ref.shape[0] // tiles
    me = lax.axis_index("band")
    core = lax.rem(me, 2)
    x = me // 2
    chips = bands // 2
    partner = x * 2 + 1 - core
    half = g_ref.shape[1] // 2
    rows = half // parts
    barrier = pltpu.get_barrier_semaphore()
    for o in range(1, bands):
        pl.semaphore_signal(barrier, inc=1, device_id={"band": lax.rem(me + o, bands)}, device_id_type=MESH)
    for o in range(1, tiles):
        pl.semaphore_signal(barrier, inc=1, device_id={"tile": lax.rem(spot + o, tiles)}, device_id_type=MESH)
    pl.semaphore_wait(barrier, bands + tiles - 2)

    def chunk(c, q):
        return pl.ds(pl.multiple_of(c * half + q * rows, SUB), rows)

    sends = []
    for q in range(parts):
        copy = pltpu.make_async_remote_copy(
            src_ref=g_ref.at[:, chunk(1 - core, q), :], dst_ref=r1.at[q],
            send_sem=s1.at[q], recv_sem=v1.at[q], device_id={"band": partner}, device_id_type=MESH)
        copy.start()
        sends.append(copy)
    first = list(sends)
    for o in range(1, tiles):
        to = lax.rem(spot + o, tiles)
        copy = pltpu.make_async_remote_copy(
            src_ref=src_ref.at[pl.ds(to * slots, slots)], dst_ref=land.at[pl.ds(spot * slots, slots)],
            send_sem=st.at[o], recv_sem=vt.at[o], device_id={"tile": to}, device_id_type=MESH)
        copy.start()
        sends.append(copy)
    land[pl.ds(spot * slots, slots)] = src_ref[pl.ds(spot * slots, slots)]
    for o in range(1, bands):
        to = lax.rem(me + o, bands)
        copy = pltpu.make_async_remote_copy(
            src_ref=a_ref.at[pl.ds(0, SUB)], dst_ref=ar.at[me], send_sem=sa.at[o], recv_sem=va.at[o],
            device_id={"band": to}, device_id_type=MESH)
        copy.start()
        sends.append(copy)
    ar[me] = a_ref[pl.ds(0, SUB), :]
    for q in range(parts):
        first[q].wait_recv()
        r2[x, q] = g_ref[:, chunk(core, q), :] + r1[q]
        for o in range(1, chips):
            to = lax.rem(x + o, chips)
            copy = pltpu.make_async_remote_copy(
                src_ref=r2.at[x, q], dst_ref=r2.at[x, q], send_sem=s2.at[o, q], recv_sem=v2.at[o, q],
                device_id={"band": to * 2 + core}, device_id_type=MESH)
            copy.start()
            sends.append(copy)
    last = []
    pair = None
    for q in range(parts):
        if q == parts // 2:
            for o in range(1, tiles):
                frm = lax.rem(spot - o + tiles, tiles)
                pltpu.make_async_remote_copy(
                    src_ref=src_ref.at[pl.ds(frm * slots, slots)], dst_ref=land.at[pl.ds(frm * slots, slots)],
                    send_sem=st.at[o], recv_sem=vt.at[o], device_id={"tile": frm},
                    device_id_type=MESH).wait_recv()
            pair = pltpu.make_async_remote_copy(
                src_ref=land, dst_ref=b1, send_sem=sb.at[0], recv_sem=vb.at[0],
                device_id={"band": partner}, device_id_type=MESH)
            pair.start()
            sends.append(pair)
            own_ref[...] = land[...]
        if q == parts - 1:
            pair.wait_recv()
            b2[x] = land[...] + b1[...]
            for o in range(1, chips):
                to = lax.rem(x + o, chips)
                copy = pltpu.make_async_remote_copy(
                    src_ref=b2.at[x], dst_ref=b2.at[x], send_sem=sc.at[o], recv_sem=vc.at[o],
                    device_id={"band": to * 2 + core}, device_id_type=MESH)
                copy.start()
                sends.append(copy)
        for o in range(1, chips):
            frm = lax.rem(x - o + chips, chips)
            pltpu.make_async_remote_copy(
                src_ref=r2.at[frm, q], dst_ref=r2.at[frm, q], send_sem=s2.at[o, q], recv_sem=v2.at[o, q],
                device_id={"band": frm * 2 + core}, device_id_type=MESH).wait_recv()
        total = r2[0, q]
        for i in range(1, chips):
            total = total + r2[i, q]
        gout_ref[:, chunk(core, q), :] = total
        copy = pltpu.make_async_remote_copy(
            src_ref=gout_ref.at[:, chunk(core, q), :], dst_ref=r3.at[q],
            send_sem=s3.at[q], recv_sem=v3.at[q], device_id={"band": partner}, device_id_type=MESH)
        copy.start()
        last.append(copy)
    for o in range(1, bands):
        frm = lax.rem(me - o + bands, bands)
        pltpu.make_async_remote_copy(
            src_ref=a_ref.at[pl.ds(0, SUB)], dst_ref=ar.at[frm], send_sem=sa.at[o], recv_sem=va.at[o],
            device_id={"band": frm}, device_id_type=MESH).wait_recv()
    total = ar[0]
    for i in range(1, bands):
        total = total + ar[i]
    aout_ref[...] = total
    for o in range(1, chips):
        frm = lax.rem(x - o + chips, chips)
        pltpu.make_async_remote_copy(
            src_ref=b2.at[frm], dst_ref=b2.at[frm], send_sem=sc.at[o], recv_sem=vc.at[o],
            device_id={"band": frm * 2 + core}, device_id_type=MESH).wait_recv()
    total = b2[0]
    for i in range(1, chips):
        total = total + b2[i]
    sum_ref[...] = total
    for q in range(parts):
        last[q].wait_recv()
        gout_ref[:, chunk(1 - core, q), :] = r3[q]
    for copy in sends + last:
        copy.wait_send()


def band_sum(packets, grad, aux, tiles, bands, cid):
    sources, pixels, lanes = grad.shape
    parts = 4
    rows = pixels // 2 // parts
    chips = bands // 2
    dma = pltpu.SemaphoreType.DMA
    return pl.pallas_call(
        functools.partial(reduce_kernel, tiles, bands, parts),
        out_shape=[jax.ShapeDtypeStruct(grad.shape, F32), jax.ShapeDtypeStruct((SUB, lanes), F32),
                   jax.ShapeDtypeStruct(packets.shape, F32), jax.ShapeDtypeStruct(packets.shape, F32)],
        in_specs=[VM] * 3, out_specs=[VM] * 4,
        scratch_shapes=[pltpu.VMEM((parts, sources, rows, lanes), F32),
                        pltpu.VMEM((chips, parts, sources, rows, lanes), F32),
                        pltpu.VMEM((parts, sources, rows, lanes), F32),
                        pltpu.VMEM((bands, SUB, lanes), F32),
                        pltpu.VMEM(packets.shape, F32), pltpu.VMEM(packets.shape, F32),
                        pltpu.VMEM((chips,) + packets.shape, F32),
                        dma((parts,)), dma((parts,)), dma((chips, parts)), dma((chips, parts)),
                        dma((parts,)), dma((parts,)), dma((bands,)), dma((bands,)), dma((tiles,)), dma((tiles,)),
                        dma((1,)), dma((1,)), dma((chips,)), dma((chips,))],
        compiler_params=pltpu.CompilerParams(collective_id=cid, has_side_effects=True),
    )(packets, grad, aux)


def step_kernel(final, chan, sent_ref, shape_ref, grad_ref, auxt_ref, cntb_ref, memt_ref, color_ref,
                sum_ref, own_ref, pb_ref, aux_ref, amask_ref, snext_ref, cnext_ref, *outs):
    sources = shape_ref.shape[0]
    slots = sum_ref.shape[0]
    sent = sent_ref[...][:slots]
    memt = memt_ref[...]
    per_block = pb_ref[...] + select_dot(own_ref[:, sources, :], sent, TN)
    grad_color = select_dot(per_block, memt, NN)
    powers = select_dot(aux_ref[pl.ds(SUB, SUB), :], memt, NN)
    row = lax.broadcasted_iota(jnp.int32, color_ref.shape, 0) // chan
    power = jnp.zeros(color_ref.shape, F32)
    for k in range(sources):
        power = jnp.where(row == k, powers[k:k + 1], power)
    color = jnp.maximum(color_ref[...] - grad_color / (1.0 + power), 0.0) * amask_ref[...]
    cnext_ref[...] = color
    for k in range(sources):
        step = 1.0 / (1.0 + auxt_ref[pl.ds(k, 1), :])
        alive = jnp.where(cntb_ref[pl.ds(0, 1), :] > k, 1.0, 0.0)
        grad = grad_ref[k] + select_dot(sum_ref[:, k, :], sent, TN)
        shape = jnp.maximum(shape_ref[k] - step * grad, 0.0) * alive
        snext_ref[k] = jnp.transpose(shape) if final else shape
    if final:
        outs[0][...] = select_dot(auxt_ref[...], memt, NN)
    else:
        outs[0][...] = select_dot(color, memt, NT)
        write_packets(sent_ref, snext_ref, outs[0], outs[1])


def on_device(
    observed, weights, morphology, spectra, blend_blocks, source_count, sent_blocks, landing_blocks
):
    chan, blocks, pixels = observed.shape
    sources = morphology.shape[0]
    blends = spectra.shape[2]
    tiles = lax.axis_size("tile")
    bands = lax.axis_size("band")
    slots = tiles * sent_blocks.shape[2]

    def onehot(index):
        index = jnp.pad(index.reshape(-1), (0, LANES - slots), constant_values=blocks)
        return (index[:, None] == jnp.arange(blocks, dtype=jnp.int32)[None, :]).astype(BF)

    sent = onehot(sent_blocks)
    hit = onehot(landing_blocks)
    spec2 = jnp.pad(spectra.reshape(sources * chan, blends), ((0, LANES - sources * chan), (0, 0)))
    sds = jax.ShapeDtypeStruct
    packet = sds((slots, SUB, LANES), F32)
    table = sds((LANES, blocks), F32)
    palette = sds((LANES, blends), F32)
    turned = sds((sources, pixels, blocks), F32)
    shape_now, color_now, cb, memt, cntb, amask, packets = pl.pallas_call(
        functools.partial(start_kernel, chan),
        in_specs=[VM] * 5, out_specs=[VM] * 7,
        out_shape=[turned, palette, table, sds((blocks, blends), BF), sds((SUB, blocks), F32), palette, packet],
    )(sent, morphology, spec2, blend_blocks, source_count.reshape(1, blends))
    for it in range(ITERS):
        recv = exchange(packets, tiles, 2 * it)
        grad, pb, aux, ret = main_pass(hit, recv, observed, weights, shape_now, cb)
        grad, auxt, back_sum, back = band_sum(ret, grad, aux, tiles, bands, 2 * it + 1)
        final = it == ITERS - 1
        if final:
            outs = [sds(morphology.shape, F32), palette, sds((SUB, blends), F32)]
        else:
            outs = [turned, palette, table, packet]
        results = pl.pallas_call(
            functools.partial(step_kernel, final, chan),
            in_specs=[VM] * 12, out_specs=[VM] * len(outs), out_shape=outs,
        )(sent, shape_now, grad, auxt, cntb, memt, color_now, back_sum, back, pb, aux, amask)
        color_now = results[1]
        if not final:
            shape_now, _, cb, packets = results
    spectra_out = color_now[:sources * chan].reshape(sources, chan, blends)
    return (results[0], spectra_out, results[2][sources])


def solution(mesh):
    return jax.shard_map(
        on_device,
        mesh=mesh,
        in_specs=(
            P("band", "tile", None),
            P("band", "tile", None),
            P(None, "tile", None),
            P(None, "band", "tile"),
            P("tile", None),
            P("tile"),
            P("tile", None, None),
            P("tile", None, None),
        ),
        out_specs=(P(None, "tile", None), P(None, "band", "tile"), P("tile")),
        check_vma=False,
    )
```
